256 devices in a mesh: stage: 64 (over z, y, core), expert: 4 (over x).
Axes of the slice: x: 4, y: 4, z: 8, core: 2. Of those that a mesh axis runs over, the one named last changes fastest.
Arguments:
- x_act: bfloat16 [64, 8192, 128], P('stage', 'expert')
- route_idx: int32 [64, 8192, 4], P('stage', 'expert')
- route_wts: float32 [64, 8192, 4], P('stage', 'expert')
- w_one: bfloat16 [64, 16, 128, 512], P('stage', 'expert')
- w_three: bfloat16 [64, 16, 128, 512], P('stage', 'expert')
- w_two: bfloat16 [64, 16, 512, 128], P('stage', 'expert')
- dy_act: bfloat16 [64, 8192, 128], P('stage', 'expert')
Outputs:
- output 1: bfloat16 [64, 8192, 128], P('stage', 'expert')
- output 2: bfloat16 [64, 8192, 128], P('stage', 'expert')
- output 3: bfloat16 [64, 16, 128, 512], P('stage', 'expert')
- output 4: bfloat16 [64, 16, 128, 512], P('stage', 'expert')
- output 5: bfloat16 [64, 16, 512, 128], P('stage', 'expert')
All inputs are finite; a program needn't handle non-finite values.
Results may differ from the reference program's by a relative error of at most 0.0125934.
Values are sent between devices in bfloat16 or wider.
A program may use at most 768 MiB of HBM per device.

```python
import jax
import jax.numpy as jnp
from jax import lax

STAGES = 64
EXPERT_DEVS = 4
TOK_DEV = 2048
MODEL_DIM = 128
FFN_DIM = 512
EXPERTS = 16
TOP_K = 4
ROUTE_DEVS = 4

LOCAL_EXP = EXPERTS // EXPERT_DEVS
CAPACITY = 2 * TOK_DEV * TOP_K // EXPERTS - 1
TOKENS = EXPERT_DEVS * TOK_DEV
N_SLOT = TOK_DEV * TOP_K


def draw_routing(rng_key):
    n_blocks = EXPERTS // TOP_K
    mean_load = TOK_DEV * TOP_K // EXPERTS
    group_devs = min(ROUTE_DEVS, EXPERT_DEVS)
    group_exp = group_devs * LOCAL_EXP
    key_pair, key_shift, key_tok, key_grp, key_dev = jax.random.split(rng_key, 5)
    block_ids = jnp.broadcast_to(jnp.arange(n_blocks, dtype=jnp.int32), (STAGES, n_blocks))
    pair_perm = jax.random.permutation(key_pair, block_ids, axis=1, independent=True)
    shifts = jax.random.randint(key_shift, (STAGES, EXPERT_DEVS, n_blocks // 2), 0, mean_load)
    shifts = shifts.at[:, :, 0].set(mean_load - 1)
    pair_sign = jnp.array([1, -1], dtype=jnp.int32)
    delta_pos = (shifts[:, :, :, None] * pair_sign).reshape(STAGES, EXPERT_DEVS, n_blocks)
    inv_perm = jnp.broadcast_to(jnp.argsort(pair_perm, axis=1)[:, None, :], delta_pos.shape)
    blk_load = mean_load + jnp.take_along_axis(delta_pos, inv_perm, axis=2)
    blk_ends = jnp.cumsum(blk_load, axis=2)
    tok_pos = jnp.arange(TOK_DEV, dtype=jnp.int32)
    blk_of = jnp.sum((blk_ends[:, :, None, :] <= tok_pos[None, None, :, None]).astype(jnp.int32), axis=3)
    blk_of = jax.random.permutation(key_tok, blk_of, axis=2, independent=True)
    virt_ids = blk_of[:, :, :, None] * TOP_K + jnp.arange(TOP_K, dtype=jnp.int32)
    virt_flat = virt_ids.reshape(STAGES, TOKENS * TOP_K)
    inner_ids = jnp.broadcast_to(jnp.arange(group_exp, dtype=jnp.int32), (STAGES, EXPERTS // group_exp, group_exp))
    grp_perm = jax.random.permutation(key_grp, inner_ids, axis=2, independent=True).reshape(STAGES, EXPERTS)
    dev_ids = jnp.broadcast_to(jnp.arange(EXPERT_DEVS, dtype=jnp.int32), (STAGES, EXPERT_DEVS))
    dev_perm = jax.random.permutation(key_dev, dev_ids, axis=1, independent=True)
    in_group = jnp.take_along_axis(grp_perm, virt_flat, axis=1)
    pre_dev = (virt_flat // group_exp) * group_devs + in_group // LOCAL_EXP
    dest_dev = jnp.take_along_axis(dev_perm, pre_dev, axis=1)
    expert_id = dest_dev * LOCAL_EXP + in_group % LOCAL_EXP
    return expert_id.reshape(STAGES, TOKENS, TOP_K)


def setup_inputs(seed: int = 0) -> dict:
    rng_key = jax.random.key(seed)
    key_x, key_idx, key_wts, key_one, key_three, key_two, key_dy = jax.random.split(rng_key, 7)
    x_act = jax.random.normal(key_x, (STAGES, TOKENS, MODEL_DIM), jnp.float32)
    route_idx = draw_routing(key_idx)
    route_wts = jax.random.uniform(key_wts, (STAGES, TOKENS, TOP_K), jnp.float32, 0.5, 1.5)
    w_one = jax.random.normal(key_one, (STAGES, EXPERTS, MODEL_DIM, FFN_DIM), jnp.float32) * MODEL_DIM ** -0.5
    w_three = jax.random.normal(key_three, (STAGES, EXPERTS, MODEL_DIM, FFN_DIM), jnp.float32) * MODEL_DIM ** -0.5
    w_two = jax.random.normal(key_two, (STAGES, EXPERTS, FFN_DIM, MODEL_DIM), jnp.float32) * FFN_DIM ** -0.5
    dy_act = jax.random.normal(key_dy, (STAGES, TOKENS, MODEL_DIM), jnp.float32)
    return {
        'x_act': x_act.astype(jnp.bfloat16),
        'route_idx': route_idx,
        'route_wts': route_wts,
        'w_one': w_one.astype(jnp.bfloat16),
        'w_three': w_three.astype(jnp.bfloat16),
        'w_two': w_two.astype(jnp.bfloat16),
        'dy_act': dy_act.astype(jnp.bfloat16),
    }


def take_rows(row_table, row_ids):
    return jnp.take(row_table, row_ids, axis=0, mode='fill', fill_value=0)


def stage_tables(idx_blk):
    slot_ids = idx_blk.reshape(N_SLOT)
    hit_mat = (slot_ids[:, None] == jnp.arange(EXPERTS, dtype=jnp.int32)[None, :]).astype(jnp.int32)
    slot_rank = jnp.sum(jnp.cumsum(hit_mat, axis=0) * hit_mat, axis=1) - 1
    buf_pos = slot_ids * CAPACITY + slot_rank
    slot_at = jnp.full((EXPERTS * CAPACITY,), N_SLOT, jnp.int32).at[buf_pos].set(jnp.arange(N_SLOT, dtype=jnp.int32))
    return buf_pos, slot_at


def one_expert(operands):
    x_rows, d_rows, w_in_one, w_in_three, w_out = operands
    pre_one = jnp.dot(x_rows, w_in_one, preferred_element_type=jnp.float32)
    pre_three = jnp.dot(x_rows, w_in_three, preferred_element_type=jnp.float32)
    sig_one = jax.nn.sigmoid(pre_one)
    act_one = pre_one * sig_one
    hidden = (act_one * pre_three).astype(jnp.bfloat16)
    out_rows = jnp.dot(hidden, w_out, preferred_element_type=jnp.float32).astype(jnp.bfloat16)
    d_hidden = jnp.dot(d_rows, w_out.T, preferred_element_type=jnp.float32).astype(jnp.bfloat16).astype(jnp.float32)
    d_three = (d_hidden * act_one).astype(jnp.bfloat16)
    d_one = (d_hidden * pre_three * sig_one * (1.0 + pre_one * (1.0 - sig_one))).astype(jnp.bfloat16)
    dx_rows = (jnp.dot(d_one, w_in_one.T, preferred_element_type=jnp.float32) + jnp.dot(d_three, w_in_three.T, preferred_element_type=jnp.float32)).astype(jnp.bfloat16)
    g_one = jnp.dot(x_rows.T, d_one, preferred_element_type=jnp.float32).astype(jnp.bfloat16)
    g_three = jnp.dot(x_rows.T, d_three, preferred_element_type=jnp.float32).astype(jnp.bfloat16)
    g_two = jnp.dot(hidden.T, d_rows, preferred_element_type=jnp.float32).astype(jnp.bfloat16)
    return out_rows, dx_rows, g_one, g_three, g_two


def to_experts(rows):
    return jnp.transpose(rows.reshape(EXPERT_DEVS, EXPERTS, CAPACITY, MODEL_DIM), (1, 0, 2, 3)).reshape(EXPERTS, EXPERT_DEVS * CAPACITY, MODEL_DIM)


def from_experts(rows):
    return jnp.transpose(rows.reshape(EXPERTS, EXPERT_DEVS, CAPACITY, MODEL_DIM), (1, 0, 2, 3)).reshape(EXPERT_DEVS, EXPERTS * CAPACITY, MODEL_DIM)


def stage_layer(operands):
    x_in, idx_in, wts_in, w_one, w_three, w_two, dy_in = operands
    buf_pos, slot_at = lax.map(stage_tables, idx_in.reshape(EXPERT_DEVS, TOK_DEV, TOP_K))
    x_dev = x_in.reshape(EXPERT_DEVS, TOK_DEV, MODEL_DIM)
    wts_dev = wts_in.reshape(EXPERT_DEVS, TOK_DEV, TOP_K)
    dy_dev = dy_in.reshape(EXPERT_DEVS, TOK_DEV, 1, MODEL_DIM)
    d_slot = (wts_dev[:, :, :, None] * dy_dev.astype(jnp.float32)).astype(jnp.bfloat16).reshape(EXPERT_DEVS, N_SLOT, MODEL_DIM)
    x_exp = to_experts(jax.vmap(take_rows)(x_dev, slot_at // TOP_K))
    d_exp = to_experts(jax.vmap(take_rows)(d_slot, slot_at))
    out_exp, dx_exp, dw_one, dw_three, dw_two = lax.map(one_expert, (x_exp, d_exp, w_one, w_three, w_two))
    out_slot = jax.vmap(take_rows)(from_experts(out_exp), buf_pos).reshape(EXPERT_DEVS, TOK_DEV, TOP_K, MODEL_DIM)
    dx_slot = jax.vmap(take_rows)(from_experts(dx_exp), buf_pos).reshape(EXPERT_DEVS, TOK_DEV, TOP_K, MODEL_DIM)
    y_out = jnp.sum(wts_dev[:, :, :, None] * out_slot.astype(jnp.float32), axis=2).astype(jnp.bfloat16)
    dx_out = jnp.sum(dx_slot.astype(jnp.float32), axis=2).astype(jnp.bfloat16)
    return y_out.reshape(TOKENS, MODEL_DIM), dx_out.reshape(TOKENS, MODEL_DIM), dw_one, dw_three, dw_two


def reference(x_act, route_idx, route_wts, w_one, w_three, w_two, dy_act):
    x_in = jnp.roll(x_act, 1, axis=0)
    idx_in = jnp.roll(route_idx, 1, axis=0)
    wts_in = jnp.roll(route_wts, 1, axis=0)
    y_act, dx_dst, dw_one, dw_three, dw_two = lax.map(stage_layer, (x_in, idx_in, wts_in, w_one, w_three, w_two, dy_act))
    dx_act = jnp.roll(dx_dst, -1, axis=0)
    return (y_act, dx_act, dw_one, dw_three, dw_two)
```

```python
import functools

import jax
import jax.numpy as jnp
from jax import lax
from jax.experimental import pallas as pl
from jax.experimental.pallas import tpu as pltpu
from jax.sharding import PartitionSpec as P

F32, BF16 = jnp.float32, jnp.bfloat16
NT = (((1,), (1,)), ((), ()))
ROW_TILE = 512
TOK_TILE = 512


def dot(a, b):
    return jnp.dot(a, b, preferred_element_type=F32)


def dot_nt(a, b):
    return lax.dot_general(a, b, NT, preferred_element_type=F32)


def sigmoid(a):
    return 0.5 + 0.5 * jnp.tanh(0.5 * a)


def local_kernel(xf_ref, xb_ref, dy_ref, gate_ref, w1_ref, w3_ref, w2_ref, y_ref, dx_ref, y_acc, dx_acc):
    e = pl.program_id(0)
    n_tok, model_dim = xf_ref.shape

    @pl.when(e == 0)
    def _():
        y_acc[...] = jnp.zeros_like(y_acc)
        dx_acc[...] = jnp.zeros_like(dx_acc)

    def tile(r, _):
        rows = pl.ds(pl.multiple_of(r * ROW_TILE, ROW_TILE), ROW_TILE)
        gate = jnp.broadcast_to(gate_ref[0, :, rows], (model_dim, ROW_TILE)).T
        w1, w3, w2 = w1_ref[0], w3_ref[0], w2_ref[0]
        a1, a3 = dot(xf_ref[rows], w1), dot(xf_ref[rows], w3)
        h = (a1 * sigmoid(a1) * a3).astype(BF16)
        y_acc[rows] += gate * dot(h, w2).astype(BF16).astype(F32)
        d = (gate * dy_ref[rows].astype(F32)).astype(BF16)
        b1, b3 = dot(xb_ref[rows], w1), dot(xb_ref[rows], w3)
        dh = dot_nt(d, w2).astype(BF16).astype(F32)
        sg = sigmoid(b1)
        act = b1 * sg
        d3 = (dh * act).astype(BF16)
        d1 = (dh * b3 * (sg + act * (1.0 - sg))).astype(BF16)
        dx_acc[rows] += (dot_nt(d1, w1) + dot_nt(d3, w3)).astype(BF16).astype(F32)
        return 0

    lax.fori_loop(0, n_tok // ROW_TILE, tile, 0)

    @pl.when(e == pl.num_programs(0) - 1)
    def _():
        y_ref[...] = y_acc[...].astype(BF16)
        dx_ref[...] = dx_acc[...].astype(BF16)


def owner_kernel(x_ref, dy_ref, gate_ref, w1_ref, w3_ref, w2_ref, g1_ref, g3_ref, g2_ref, w1t, w3t, acc1, acc3, acc2):
    i = pl.program_id(0)
    n_local = w1_ref.shape[0]

    @pl.when(i == 0)
    def _():
        for e in range(n_local):
            w1t[e] = w1_ref[e].T
            w3t[e] = w3_ref[e].T
        acc1[...] = jnp.zeros_like(acc1)
        acc3[...] = jnp.zeros_like(acc3)
        acc2[...] = jnp.zeros_like(acc2)

    x_t = x_ref[...].T
    dy_t = dy_ref[...].astype(F32).T

    def expert(e, _):
        d_t = (gate_ref[e] * dy_t).astype(BF16)
        a1, a3 = dot(w1t[e], x_t), dot(w3t[e], x_t)
        dh = dot(w2_ref[e], d_t).astype(BF16).astype(F32)
        sg = sigmoid(a1)
        act = a1 * sg
        h = (act * a3).astype(BF16)
        d3 = (dh * act).astype(BF16)
        d1 = (dh * a3 * (sg + act * (1.0 - sg))).astype(BF16)
        acc1[e] += dot_nt(d1, x_t)
        acc3[e] += dot_nt(d3, x_t)
        acc2[e] += dot_nt(h, d_t)
        return 0

    lax.fori_loop(0, n_local, expert, 0)

    @pl.when(i == pl.num_programs(0) - 1)
    def _():
        for e in range(n_local):
            g1_ref[e] = acc1[e].T.astype(BF16)
            g3_ref[e] = acc3[e].T.astype(BF16)
            g2_ref[e] = acc2[e].astype(BF16)


def local_call(x_f, x_b, dy, gates, w1, w3, w2):
    n_tok, model_dim = x_f.shape
    n_exp, _, ffn = w1.shape
    whole = pl.BlockSpec((n_tok, model_dim), lambda e: (0, 0))
    return pl.pallas_call(
        local_kernel,
        grid=(n_exp,),
        in_specs=[whole, whole, whole, pl.BlockSpec((1, 1, n_tok), lambda e: (e, 0, 0)), pl.BlockSpec((1, model_dim, ffn), lambda e: (e, 0, 0)), pl.BlockSpec((1, model_dim, ffn), lambda e: (e, 0, 0)), pl.BlockSpec((1, ffn, model_dim), lambda e: (e, 0, 0))],
        out_specs=[whole, whole],
        out_shape=[jax.ShapeDtypeStruct((n_tok, model_dim), BF16)] * 2,
        scratch_shapes=[pltpu.VMEM((n_tok, model_dim), F32)] * 2,
        cost_estimate=pl.CostEstimate(flops=16 * n_tok * n_exp * model_dim * ffn, bytes_accessed=8 << 20, transcendentals=0),
        compiler_params=pltpu.CompilerParams(vmem_limit_bytes=56 << 20),
        name='local_rows',
    )(x_f, x_b, dy, gates[:, None, :], w1, w3, w2)


def owner_call(x_all, dy_all, gates, w1, w3, w2):
    n_tok, model_dim = x_all.shape
    n_local, _, ffn = w1.shape
    toks = pl.BlockSpec((TOK_TILE, model_dim), lambda i: (i, 0))
    w_in = pl.BlockSpec((n_local, model_dim, ffn), lambda i: (0, 0, 0))
    w_out = pl.BlockSpec((n_local, ffn, model_dim), lambda i: (0, 0, 0))
    return pl.pallas_call(
        owner_kernel,
        grid=(n_tok // TOK_TILE,),
        in_specs=[toks, toks, pl.BlockSpec((n_local, 1, TOK_TILE), lambda i: (0, 0, i)), w_in, w_in, w_out],
        out_specs=[w_in, w_in, w_out],
        out_shape=[jax.ShapeDtypeStruct(w1.shape, BF16), jax.ShapeDtypeStruct(w3.shape, BF16), jax.ShapeDtypeStruct(w2.shape, BF16)],
        scratch_shapes=[pltpu.VMEM((n_local, ffn, model_dim), BF16)] * 2 + [pltpu.VMEM((n_local, ffn, model_dim), F32)] * 3,
        cost_estimate=pl.CostEstimate(flops=12 * n_tok * n_local * model_dim * ffn, bytes_accessed=8 << 20, transcendentals=0),
        compiler_params=pltpu.CompilerParams(vmem_limit_bytes=56 << 20),
        name='owner_grads',
    )(x_all, dy_all, gates, w1, w3, w2)


def solution(mesh):
    n_stage = mesh.shape['stage']
    n_dev = mesh.shape['expert']
    to_next = [(i, (i + 1) % n_stage) for i in range(n_stage)]
    to_prev = [((i + 1) % n_stage, i) for i in range(n_stage)]
    tok_spec = P('stage', 'expert', None)
    w_spec = P('stage', 'expert', None, None)

    def moe_layer(x_act, route_idx, route_wts, w_one, w_three, w_two, dy_act):
        x_src, dy = x_act[0], dy_act[0]
        n_tok = x_src.shape[0]
        n_local = w_one.shape[1]
        n_exp = n_local * n_dev
        w1, w3, w2 = w_one[0], w_three[0], w_two[0]

        idx = lax.ppermute(route_idx[0].T, 'stage', to_next)
        wts = lax.ppermute(route_wts[0].T, 'stage', to_next)
        x_f = lax.ppermute(x_src, 'stage', to_next)
        x_again, x_f = lax.optimization_barrier((x_src, x_f))
        x_b = lax.ppermute(x_again, 'stage', to_next)

        hit = idx[None, :, :] == jnp.arange(n_exp, dtype=jnp.int32)[:, None, None]
        gates = jnp.sum(jnp.where(hit, wts[None], 0.0), axis=1)
        my_gates = lax.all_to_all(gates.reshape(n_dev, n_local, n_tok), 'expert', 0, 0)
        my_gates = jnp.transpose(my_gates, (1, 0, 2)).reshape(n_local, 1, n_dev * n_tok)

        gather = functools.partial(lax.all_gather, axis_name='expert', axis=0, tiled=True)
        dy_all, x_all = gather(dy), gather(x_b)
        w1_all, w3_all, w2_all = gather(w1), gather(w3), gather(w2)

        g_one, g_three, g_two = owner_call(x_all, dy_all, my_gates, w1, w3, w2)
        y, dx = local_call(x_f, x_b, dy, gates, w1_all, w3_all, w2_all)
        dx_src = lax.ppermute(dx, 'stage', to_prev)
        return y[None], dx_src[None], g_one[None], g_three[None], g_two[None]

    return jax.shard_map(moe_layer, mesh=mesh, in_specs=(tok_spec, tok_spec, tok_spec, w_spec, w_spec, w_spec, tok_spec), out_specs=(tok_spec, tok_spec, w_spec, w_spec, w_spec), check_vma=False)
```

```python
import functools

import jax
import jax.numpy as jnp
from jax import lax
from jax.experimental import pallas as pl
from jax.experimental.pallas import tpu as pltpu
from jax.sharding import PartitionSpec as P

F32, BF16, I32 = jnp.float32, jnp.bfloat16, jnp.int32
NT = (((1,), (1,)), ((), ()))
TILE = 256
CHUNK = 256
LANES = 128
PAY_ROWS = 8
N_DEV = 4


def dot(a, b):
    return jnp.dot(a, b, preferred_element_type=F32)


def dot_nt(a, b):
    return lax.dot_general(a, b, NT, preferred_element_type=F32)


def sigmoid(a):
    return 0.5 + 0.5 * jnp.tanh(0.5 * a)


def iota(shape, axis):
    return lax.broadcasted_iota(I32, shape, axis)


def ones_where(cond):
    return jnp.where(cond, 1.0, 0.0)


def rank_kernel(n_local, me_ref, aux_ref, cols_ref, rank_ref, key_col):
    top_k, n_tok = aux_ref.shape[0] // 2, aux_ref.shape[1]
    n_exp = N_DEV * n_local
    idx, wts = aux_ref[:top_k].astype(I32), aux_ref[top_k:]
    mask = jnp.sum(jnp.left_shift(jnp.ones_like(idx), idx), axis=0, keepdims=True)
    key = mask * n_tok + iota((1, n_tok), 1)
    key_col[...] = jnp.broadcast_to(key, (LANES, n_tok)).T

    row = iota((n_exp, n_tok), 0)
    slot = row // n_local
    ahead = jnp.where(slot == 0, 0, jnp.where(slot == 1, N_DEV - 1, slot - 1))
    exp_id = lax.rem(me_ref[0] + ahead, N_DEV) * n_local + lax.rem(row, n_local)
    gate = jnp.zeros((n_exp, n_tok), F32)
    for j in range(top_k):
        gate = gate + jnp.where(exp_id == idx[j:j + 1], wts[j:j + 1], 0.0)
    high = gate.astype(BF16).astype(F32)
    rest = gate - high
    mid = rest.astype(BF16).astype(F32)
    parts = jnp.concatenate([high, mid, rest - mid, jnp.zeros((LANES - 3 * n_exp, n_tok), F32)], axis=0)
    cols_ref[...] = parts.T.astype(BF16)

    def count(c, ranks):
        col = key_col[pl.ds(pl.multiple_of(c * CHUNK, CHUNK), CHUNK), :]
        return tuple(r + jnp.sum((col < key[:, j * LANES:(j + 1) * LANES]).astype(I32), axis=0, keepdims=True) for j, r in enumerate(ranks))

    ranks = lax.fori_loop(0, n_tok // CHUNK, count, tuple(jnp.zeros((1, LANES), I32) for _ in range(n_tok // LANES)))
    rank_ref[...] = jnp.concatenate(ranks, axis=1)


def item_lists(hit, n_local, n_tile, same, place):
    n_exp = hit.shape[0]
    lane = iota((n_exp, LANES), 1).astype(F32)
    row_a, row_b = iota((n_exp, n_exp), 0), iota((n_exp, n_exp), 1)
    lane_a, lane_b = iota((LANES, LANES), 0), iota((LANES, LANES), 1)
    in_row = dot(hit, ones_where(lane_a < lane_b))
    per_row = dot(hit, jnp.ones((LANES, LANES), F32))
    ahead_of = in_row + dot(same * ones_where(row_b < row_a), per_row)
    total = dot(same, per_row)
    item = place * n_tile + lane
    pos = jnp.where(hit > 0.0, ahead_of, total + item - ahead_of)
    found = jnp.zeros((n_exp, LANES), F32)
    for t in range(n_tile):
        found = found + jnp.where(jnp.broadcast_to(pos[:, t:t + 1], (n_exp, LANES)) == lane, place * n_tile + t, 0.0)
    return dot(same, found), total


def sort_kernel(n_local, xf_ref, xb_ref, dy_ref, cols_ref, rank_ref, xfs_ref, xds_ref, gate_ref, pay_ref, meta_ref, table, sorted_gates):
    n_exp, _, n_tok = gate_ref.shape
    n_tile = n_tok // TILE
    model_dim = xf_ref.shape[1]
    n_half = n_tok // 2 // CHUNK
    rank = rank_ref[...]
    table[:, :model_dim] = xf_ref[...]
    table[:, model_dim:2 * model_dim] = xb_ref[...]
    table[:, 2 * model_dim:3 * model_dim] = dy_ref[...]
    table[:, 3 * model_dim:] = cols_ref[...]

    def permute(c, _):
        rows = pl.ds(pl.multiple_of(c * CHUNK, CHUNK), CHUNK)
        pick = ones_where(iota((CHUNK, n_tok), 0) + c * CHUNK == rank).astype(BF16)
        out = dot(pick, table[...])
        xfs_ref[rows] = out[:, :model_dim].astype(BF16)
        part = pl.ds(pl.multiple_of(lax.rem(c, n_half) * CHUNK, CHUNK), CHUNK)
        xds_ref[lax.div(c, n_half), 0, part] = out[:, model_dim:2 * model_dim].astype(BF16)
        xds_ref[lax.div(c, n_half), 1, part] = out[:, 2 * model_dim:3 * model_dim].astype(BF16)
        sorted_gates[rows] = out[:, 3 * model_dim:]
        return 0

    lax.fori_loop(0, n_tok // CHUNK, permute, 0)
    split = sorted_gates[...].T
    gate = split[:n_exp] + split[n_exp:2 * n_exp] + split[2 * n_exp:3 * n_exp]
    for i in range(n_exp):
        gate_ref[i] = gate[i:i + 1]

    lane = iota((n_exp, LANES), 1)
    hit = jnp.zeros((n_exp, LANES), F32)
    for t in range(n_tile):
        active = ones_where(jnp.max(gate[:, t * TILE:(t + 1) * TILE], axis=1, keepdims=True) > 0.0)
        hit = hit + jnp.where(lane == t, jnp.broadcast_to(active, (n_exp, LANES)), 0.0)
    row_a, row_b = iota((n_exp, n_exp), 0), iota((n_exp, n_exp), 1)
    row = iota((n_exp, LANES), 0)

    def group_first(r):
        return jnp.where(r < n_local, 0, jnp.where(r < 3 * n_local, n_local, 3 * n_local))

    order, total = item_lists(hit, n_local, n_tile, ones_where(group_first(row_a) == group_first(row_b)), (row - group_first(row)).astype(F32))
    meta_ref[:n_exp] = order.astype(I32)
    meta_ref[n_exp:] = total.astype(I32)
    order, total = item_lists(hit, n_local, n_tile, ones_where(row_a // n_local == row_b // n_local), lax.rem(row, n_local).astype(F32))
    pay_ref[...] = jnp.zeros_like(pay_ref)
    for s in range(n_exp // n_local):
        pay_ref[s, :n_local] = gate[s * n_local:(s + 1) * n_local]
        pay_ref[s, n_local:n_local + 1, :LANES] = order[s * n_local:s * n_local + 1]
        pay_ref[s, n_local + 1:n_local + 2, :LANES] = total[s * n_local:s * n_local + 1]


def local_kernel(n_parts, first, last, *refs):
    it = iter(refs)
    meta_ref, xf_ref, xd_ref, gate_ref = (next(it) for _ in range(4))
    parts = [next(it) for _ in range(n_parts)]
    if first == 0:
        y_in = dx_in = None
    else:
        y_in, dx_in = next(it), next(it)
    rank_ref = next(it) if last else None
    next(it)
    y_ref, dx_ref, token_ref = next(it), next(it), next(it)
    token_ref[...] = jnp.zeros_like(token_ref)
    w, sems = next(it), next(it)
    if last:
        y_acc, dx_acc, rank_col, table = (next(it) for _ in range(4))
    else:
        y_acc, dx_acc = y_ref, dx_ref
    n_tok, model_dim = xf_ref.shape
    n_exp = gate_ref.shape[0]

    copies = []
    at = 0
    for part in parts:
        n = part.shape[0]
        copies.append(pltpu.make_async_copy(part, w.at[pl.ds(at, n)], sems.at[len(copies)]))
        at += n
    for c in copies:
        c.start()
    if first == 0:
        y_acc[...] = jnp.zeros_like(y_acc)
        dx_acc[...] = jnp.zeros_like(dx_acc)
    else:
        y_acc[...] = y_in[...]
        dx_acc[...] = dx_in[...]
    for c in copies:
        c.wait()

    n_half = n_tok // 2 // TILE

    def chain(m):
        e, r = lax.div(m, n_tok // TILE), lax.rem(m, n_tok // TILE)
        rows = pl.ds(pl.multiple_of(r * TILE, TILE), TILE)
        part = pl.ds(pl.multiple_of(lax.rem(r, n_half) * TILE, TILE), TILE)
        half = lax.div(r, n_half)
        x_f, x_b, dy = xf_ref[rows], xd_ref[half, 0, part], xd_ref[half, 1, part]
        w1, w3, w2t = w[e, 0], w[e, 1], w[e, 2]
        gate = jnp.broadcast_to(gate_ref[first + e, :, rows], (model_dim, TILE)).T
        a1, a3 = dot(x_f, w1), dot(x_f, w3)
        h = (a1 * sigmoid(a1) * a3).astype(BF16)
        y = gate * dot_nt(h, w2t).astype(BF16).astype(F32)
        d = (gate * dy.astype(F32)).astype(BF16)
        b1, b3 = dot(x_b, w1), dot(x_b, w3)
        dh = dot(d, w2t).astype(BF16).astype(F32)
        sg = sigmoid(b1)
        act = b1 * sg
        d3 = (dh * act).astype(BF16)
        d1 = (dh * b3 * (sg + act * (1.0 - sg))).astype(BF16)
        dx = (dot_nt(d1, w1) + dot_nt(d3, w3)).astype(BF16).astype(F32)
        return rows, y, dx

    def pair(p, _):
        one, two = chain(meta_ref[first, 2 * p]), chain(meta_ref[first, 2 * p + 1])
        for rows, y, dx in (one, two):
            y_acc[rows] += y
            dx_acc[rows] += dx
        return 0

    lax.fori_loop(0, lax.shift_right_logical(meta_ref[n_exp + first, 0] + 1, 1), pair, 0)

    if last:
        rank_col[...] = jnp.broadcast_to(rank_ref[...], (LANES, n_tok)).T
        table[:, :model_dim] = y_acc[...].astype(BF16)
        table[:, model_dim:] = dx_acc[...].astype(BF16)

        def restore(c, _):
            rows = pl.ds(pl.multiple_of(c * CHUNK, CHUNK), CHUNK)
            col = rank_col[rows, :]
            pick = jnp.concatenate([ones_where(col == iota((CHUNK, LANES), 1) + j * LANES).astype(BF16) for j in range(n_tok // LANES)], axis=1)
            out = dot(pick, table[...])
            y_ref[rows] = out[:, :model_dim].astype(BF16)
            dx_ref[rows] = out[:, model_dim:].astype(BF16)
            return 0

        lax.fori_loop(0, n_tok // CHUNK, restore, 0)


def owner_kernel(n_src, n_half, first, last, *refs):
    it = iter(refs)
    meta_ref = next(it)
    sources = [[[next(it) for _ in range(n_half)], next(it)] for _ in range(n_src)]
    w_ref = next(it)
    acc_in = None if first else [next(it) for _ in range(3)]
    next(it)
    outs = [next(it) for _ in range(3)]
    token_ref = next(it)
    token_ref[...] = jnp.zeros_like(token_ref)
    accs = [next(it) for _ in range(3)] if last else outs
    if n_half > 1:
        joined, sems = next(it), next(it)
        copies = [pltpu.make_async_copy(ref, joined.at[pl.ds(k, 1)], sems.at[k]) for k, ref in enumerate(sources[0][0])]
        for c in copies:
            c.start()
        sources[0][0] = [joined]
    n_local = w_ref.shape[0]
    acc1, acc3, acc2 = accs

    for k, acc in enumerate(accs):
        acc[...] = jnp.zeros_like(acc) if first else acc_in[k][...]

    if n_half > 1:
        for c in copies:
            c.wait()
    for s, ((xd_ref,), pay_ref) in enumerate(sources):
        n_part = xd_ref.shape[2] // TILE
        n_tile = 2 * n_part

        def chain(m):
            e, t = lax.div(m, n_tile), lax.rem(m, n_tile)
            rows = pl.ds(pl.multiple_of(t * TILE, TILE), TILE)
            part = pl.ds(pl.multiple_of(lax.rem(t, n_part) * TILE, TILE), TILE)
            half = lax.div(t, n_part)
            x_t = xd_ref[half, 0, part].T
            d_t = (pay_ref[pl.ds(e, 1), rows] * xd_ref[half, 1, part].astype(F32).T).astype(BF16)
            a1, a3 = dot(w_ref[e, 0], x_t), dot(w_ref[e, 1], x_t)
            dh = dot(w_ref[e, 2], d_t).astype(BF16).astype(F32)
            sg = sigmoid(a1)
            act = a1 * sg
            h = (act * a3).astype(BF16)
            d3 = (dh * act).astype(BF16)
            d1 = (dh * a3 * (sg + act * (1.0 - sg))).astype(BF16)
            return e, dot_nt(d1, x_t), dot_nt(d3, x_t), dot_nt(h, d_t)

        def pair(p, _):
            one = chain(meta_ref[2 * s, 2 * p])
            two = chain(meta_ref[2 * s, 2 * p + 1])
            for e, g1, g3, g2 in (one, two):
                acc1[e] += g1
                acc3[e] += g3
                acc2[e] += g2
            return 0

        lax.fori_loop(0, lax.shift_right_logical(meta_ref[2 * s + 1, 0] + 1, 1), pair, 0)

    if last:
        for e in range(n_local):
            outs[0][e] = acc1[e].T.astype(BF16)
            outs[1][e] = acc3[e].T.astype(BF16)
            outs[2][e] = acc2[e].astype(BF16)


VMEM = pl.BlockSpec(memory_space=pltpu.VMEM)
SMEM = pl.BlockSpec(memory_space=pltpu.SMEM)
ANY = pl.BlockSpec(memory_space=pl.ANY)
TOKEN = jax.ShapeDtypeStruct((8, LANES), F32)


def params(flops):
    return dict(cost_estimate=pl.CostEstimate(flops=flops, bytes_accessed=8 << 20, transcendentals=0), compiler_params=pltpu.CompilerParams(vmem_limit_bytes=24 << 20))


def rank_call(aux, me, n_local, n_tok):
    return pl.pallas_call(
        functools.partial(rank_kernel, n_local),
        in_specs=[SMEM, VMEM],
        out_specs=[VMEM] * 2,
        out_shape=[jax.ShapeDtypeStruct((n_tok, LANES), BF16), jax.ShapeDtypeStruct((1, n_tok), I32)],
        scratch_shapes=[pltpu.VMEM((n_tok, LANES), I32)],
        name='rank_tokens',
        **params(1 << 30),
    )(me, aux)


def sort_call(x_f, x_b, dy, cols, rank, n_local):
    n_tok, model_dim = x_f.shape
    n_exp = N_DEV * n_local
    shapes = [jax.ShapeDtypeStruct((n_tok, model_dim), BF16), jax.ShapeDtypeStruct((2, 2, n_tok // 2, model_dim), BF16), jax.ShapeDtypeStruct((n_exp, 1, n_tok), F32), jax.ShapeDtypeStruct((N_DEV, PAY_ROWS, n_tok), F32), jax.ShapeDtypeStruct((2 * n_exp, LANES), I32)]
    return pl.pallas_call(
        functools.partial(sort_kernel, n_local),
        in_specs=[VMEM] * 5,
        out_specs=[VMEM] * len(shapes),
        out_shape=shapes,
        scratch_shapes=[pltpu.VMEM((n_tok, 3 * model_dim + LANES), BF16), pltpu.VMEM((n_tok, LANES), F32)],
        name='sort_tokens',
        **params(8 * n_tok * n_tok * model_dim),
    )(x_f, x_b, dy, cols, rank)


def local_call(name, meta, rows, gates, parts, first, carry, rank, after):
    n_tok, model_dim = rows[0].shape
    ffn = parts[0].shape[3]
    n_held = sum(p.shape[0] for p in parts)
    last = rank is not None
    args = [meta, *rows, gates, *parts]
    specs = [SMEM] + [VMEM] * 3 + [ANY] * len(parts)
    if carry is not None:
        args += list(carry)
        specs += [VMEM] * 2
    if last:
        args += [rank]
        specs += [VMEM]
    scratch = [pltpu.VMEM((n_held, 3, model_dim, ffn), BF16), pltpu.SemaphoreType.DMA((len(parts),))]
    if last:
        scratch += [pltpu.VMEM((n_tok, model_dim), F32)] * 2 + [pltpu.VMEM((n_tok, LANES), I32), pltpu.VMEM((n_tok, 2 * model_dim), BF16)]
    return pl.pallas_call(
        functools.partial(local_kernel, len(parts), first, last),
        in_specs=specs + [ANY],
        out_specs=[VMEM] * 3,
        out_shape=[jax.ShapeDtypeStruct((n_tok, model_dim), BF16 if last else F32)] * 2 + [TOKEN],
        scratch_shapes=scratch,
        name=name,
        **params(8 * n_tok * n_held * model_dim * ffn),
    )(*args, after)


def owner_call(name, meta, sources, weights, carry, last, after):
    n_local, _, ffn, model_dim = weights.shape
    n_half = len(sources[0][0])
    blocks = sources[0][0][0].shape
    args = [meta] + [a for s in sources for a in (*s[0], s[1])] + [weights]
    specs = [SMEM] + ([ANY] * n_half if n_half > 1 else [VMEM]) + [VMEM] * (len(args) - 1 - n_half)
    if carry is not None:
        args += list(carry)
        specs += [VMEM] * 3
    total = (n_local, ffn, model_dim)
    w_in = jax.ShapeDtypeStruct((n_local, model_dim, ffn), BF16)
    shapes = [w_in, w_in, jax.ShapeDtypeStruct(total, BF16)] if last else [jax.ShapeDtypeStruct(total, F32)] * 3
    return pl.pallas_call(
        functools.partial(owner_kernel, len(sources), n_half, carry is None, last),
        in_specs=specs + [ANY],
        out_specs=[VMEM] * 4,
        out_shape=shapes + [TOKEN],
        scratch_shapes=([pltpu.VMEM(total, F32)] * 3 if last else []) + ([pltpu.VMEM((n_half, *blocks[1:]), BF16), pltpu.SemaphoreType.DMA((n_half,))] if n_half > 1 else []),
        name=name,
        **params(6 * len(sources) * sources[0][1].shape[1] * n_local * model_dim * ffn),
    )(*args, after)


def pack_kernel(w1_ref, w3_ref, w2_ref, packed_ref, turned_ref, packed, turned, sems):
    ins = [
        pltpu.make_async_copy(w2_ref, turned.at[:, 2], sems.at[0]),
        pltpu.make_async_copy(w1_ref, packed.at[:, 0], sems.at[1]),
        pltpu.make_async_copy(w3_ref, packed.at[:, 1], sems.at[2]),
    ]
    outs = [pltpu.make_async_copy(packed, packed_ref, sems.at[3]), pltpu.make_async_copy(turned, turned_ref, sems.at[4])]
    for c in ins:
        c.start()
    ins[0].wait()
    for e in range(packed.shape[0]):
        packed[e, 2] = turned[e, 2].T
    ins[1].wait()
    ins[2].wait()
    outs[0].start()
    for e in range(packed.shape[0]):
        turned[e, 0] = packed[e, 0].T
        turned[e, 1] = packed[e, 1].T
    outs[1].start()
    for c in outs:
        c.wait()


def pack_call(w1, w3, w2):
    n, model_dim, ffn = w1.shape
    shapes = (n, 3, model_dim, ffn), (n, 3, ffn, model_dim)
    return pl.pallas_call(
        pack_kernel,
        in_specs=[ANY] * 3,
        out_specs=[ANY] * 2,
        out_shape=[jax.ShapeDtypeStruct(shape, BF16) for shape in shapes],
        scratch_shapes=[pltpu.VMEM(shape, BF16) for shape in shapes] + [pltpu.SemaphoreType.DMA((5,))],
        name='pack_weights',
        **params(1 << 20),
    )(w1, w3, w2)


def halves_kernel(*refs):
    n = (len(refs) - 1) // 2
    for src, dst in zip(refs[:n], refs[n + 1:]):
        dst[...] = src[...]


def halves_call(lefts, rights, after):
    def half(a, k):
        return pl.BlockSpec((a.shape[0] // 2, *a.shape[1:]), lambda i: (k,) + (0,) * (a.ndim - 1))

    ins = [half(a, 0) for a in lefts] + [half(a, 1) for a in rights]
    arrays = [*lefts, *rights]
    return pl.pallas_call(
        halves_kernel,
        grid=(1,),
        in_specs=ins + [ANY],
        out_specs=[half(a, 0) for a in arrays],
        out_shape=[jax.ShapeDtypeStruct((a.shape[0] // 2, *a.shape[1:]), a.dtype) for a in arrays],
        name='halves',
        **params(1 << 20),
    )(*arrays, after)


def solution(mesh):
    n_stage = mesh.shape['stage']
    n_dev = mesh.shape['expert']
    assert n_dev == N_DEV
    to_next = [(i, (i + 1) % n_stage) for i in range(n_stage)]
    to_prev = [((i + 1) % n_stage, i) for i in range(n_stage)]
    tok_spec = P('stage', 'expert', None)
    w_spec = P('stage', 'expert', None, None)

    def from_ring(a, ahead):
        return lax.ppermute(a, 'expert', [((i + ahead) % n_dev, i) for i in range(n_dev)])

    def from_sides(a):
        return from_ring(a, n_dev - 1), from_ring(a, 1)

    def from_far(sides, after):
        one, two = halves_call(sides[:1], sides[1:], after)
        return from_ring(one, n_dev - 1), from_ring(two, 1)

    def moe_layer(x_act, route_idx, route_wts, w_one, w_three, w_two, dy_act):
        x_src, dy = x_act[0], dy_act[0]
        n_local = w_one.shape[1]
        me = lax.axis_index('expert').astype(I32).reshape(1)

        aux = jnp.concatenate([route_idx[0].T.astype(F32), route_wts[0].T], axis=0)
        aux, w1 = lax.optimization_barrier((aux, w_one[0]))
        packed, turned = pack_call(w1, w_three[0], w_two[0])
        aux = lax.ppermute(aux, 'stage', to_next)
        x_b = lax.ppermute(x_src, 'stage', to_next)
        x_again, aux = lax.optimization_barrier((x_src, aux))
        x_f = lax.ppermute(x_again, 'stage', to_next)
        sides = from_sides(packed)
        cols, rank = rank_call(aux, me, n_local, x_src.shape[0])
        x_f, xd, gates, pay, meta = sort_call(x_f, x_b, dy, cols, rank, n_local)
        rows = (x_f, xd)
        pay_side = from_ring(pay[2], n_dev - 1), from_ring(pay[1], 1)
        pay_far = from_ring(pay[3], 2)
        xd_side = from_sides(xd)

        def lists(after, *pays):
            return jnp.concatenate([p[n_local:n_local + 2, :LANES] + after[:2] for p in pays], axis=0).astype(I32)

        *totals, token = local_call('local_own', meta, rows, gates, [packed], 0, None, None, rank)
        *sums, token = owner_call('owner_own', lists(token, pay[0]), [([xd], pay[0])], turned, None, False, token)
        far = from_far(sides, token)
        *totals, token = local_call('local_sides', meta, rows, gates, list(sides), n_local, totals, None, token)
        xd_far = from_far(xd_side, token)
        *sums, token = owner_call('owner_sides', lists(token, *pay_side), [([xd_side[k]], pay_side[k]) for k in range(2)], turned, sums, False, token)
        y, dx, token = local_call('local_far', meta, rows, gates, list(far), 3 * n_local, totals, rank, token)
        dx_src = lax.ppermute(dx, 'stage', to_prev)
        g_one, g_three, g_two, token = owner_call('owner_far', lists(token, pay_far), [(list(xd_far), pay_far)], turned, sums, True, token)
        return y[None], dx_src[None], g_one[None], g_three[None], g_two[None]

    return jax.shard_map(moe_layer, mesh=mesh, in_specs=(tok_spec, tok_spec, tok_spec, w_spec, w_spec, w_spec, tok_spec), out_specs=(tok_spec, tok_spec, w_spec, w_spec, w_spec), check_vma=False)
```

```python
import functools

import jax
import jax.numpy as jnp
from jax import lax
from jax.experimental import pallas as pl
from jax.experimental.pallas import tpu as pltpu
from jax.sharding import PartitionSpec as P

F32, BF16, I32 = jnp.float32, jnp.bfloat16, jnp.int32
NT = (((1,), (1,)), ((), ()))
TILE = 256
CHUNK = 256
LOCAL_BLOCKS = 3
OWNER_BLOCKS = 3
OWN_BLOCKS = 6
HEAD_BLOCKS = 24
LANES = 128
PAY_ROWS = 8
N_DEV = 4


def dot(a, b):
    return jnp.dot(a, b, preferred_element_type=F32)


def dot_nt(a, b):
    return lax.dot_general(a, b, NT, preferred_element_type=F32)


def sigmoid(a):
    return 0.5 + 0.5 * jnp.tanh(0.5 * a)


def iota(shape, axis):
    return lax.broadcasted_iota(I32, shape, axis)


def ones_where(cond):
    return jnp.where(cond, 1.0, 0.0)


def rank_kernel(n_local, me_ref, aux_ref, cols_ref, rank_ref, token_ref, key_col):
    top_k, n_tok = aux_ref.shape[0] // 2, aux_ref.shape[1]
    n_exp = N_DEV * n_local
    token_ref[...] = jnp.zeros_like(token_ref)
    idx, wts = aux_ref[:top_k].astype(I32), aux_ref[top_k:]
    mask = jnp.sum(jnp.left_shift(jnp.ones_like(idx), idx), axis=0, keepdims=True)
    key = mask * n_tok + iota((1, n_tok), 1)
    key_col[...] = jnp.broadcast_to(key, (LANES, n_tok)).T

    row = iota((n_exp, n_tok), 0)
    slot = row // n_local
    ahead = jnp.where(slot == 0, 0, jnp.where(slot == 1, N_DEV - 1, slot - 1))
    exp_id = lax.rem(me_ref[0] + ahead, N_DEV) * n_local + lax.rem(row, n_local)
    gate = jnp.zeros((n_exp, n_tok), F32)
    for j in range(top_k):
        gate = gate + jnp.where(exp_id == idx[j:j + 1], wts[j:j + 1], 0.0)
    high = gate.astype(BF16).astype(F32)
    rest = gate - high
    mid = rest.astype(BF16).astype(F32)
    parts = jnp.concatenate([high, mid, rest - mid, jnp.zeros((LANES - 3 * n_exp, n_tok), F32)], axis=0)
    cols_ref[...] = parts.T.astype(BF16)

    def count(c, ranks):
        col = key_col[pl.ds(pl.multiple_of(c * CHUNK, CHUNK), CHUNK), :]
        return tuple(r + jnp.sum((col < key[:, j * LANES:(j + 1) * LANES]).astype(I32), axis=0, keepdims=True) for j, r in enumerate(ranks))

    ranks = lax.fori_loop(0, n_tok // CHUNK, count, tuple(jnp.zeros((1, LANES), I32) for _ in range(n_tok // LANES)))
    rank_ref[...] = jnp.concatenate(ranks, axis=1)


def item_lists(hit, n_tile, same, place):
    n_exp = hit.shape[0]
    lane = iota((n_exp, LANES), 1).astype(F32)
    row_a, row_b = iota((n_exp, n_exp), 0), iota((n_exp, n_exp), 1)
    lane_a, lane_b = iota((LANES, LANES), 0), iota((LANES, LANES), 1)
    in_row = dot(hit, ones_where(lane_a < lane_b))
    per_row = dot(hit, jnp.ones((LANES, LANES), F32))
    ahead_of = in_row + dot(same * ones_where(row_b < row_a), per_row)
    total = dot(same, per_row)
    item = place * n_tile + lane
    pos = jnp.where(hit > 0.0, ahead_of, total + item - ahead_of)
    found = jnp.zeros((n_exp, LANES), F32)
    for t in range(n_tile):
        found = found + jnp.where(jnp.broadcast_to(pos[:, t:t + 1], (n_exp, LANES)) == lane, place * n_tile + t, 0.0)
    return dot(same, found), total


def order_rows(rank, table, store):
    n_tok = rank.shape[1]

    def step(c, _):
        pick = ones_where(iota((CHUNK, n_tok), 0) + c * CHUNK == rank).astype(BF16)
        store(c, dot(pick, table[...]))
        return 0

    lax.fori_loop(0, n_tok // CHUNK, step, 0)


def forward_kernel(x_ref, rank_ref, after_ref, out_ref):
    def store(c, rows):
        out_ref[pl.ds(pl.multiple_of(c * CHUNK, CHUNK), CHUNK)] = rows.astype(BF16)

    order_rows(rank_ref[...], x_ref, store)


def sort_kernel(n_local, xb_ref, dy_ref, cols_ref, rank_ref, xds_ref, gate_ref, pay_ref, meta_ref, table, sorted_gates):
    n_exp, _, n_tok = gate_ref.shape
    n_tile = n_tok // TILE
    model_dim = xb_ref.shape[1]
    n_half = n_tok // 2 // CHUNK
    table[:, :model_dim] = xb_ref[...]
    table[:, model_dim:2 * model_dim] = dy_ref[...]
    table[:, 2 * model_dim:] = cols_ref[...]

    def store(c, out):
        part = pl.ds(pl.multiple_of(lax.rem(c, n_half) * CHUNK, CHUNK), CHUNK)
        xds_ref[lax.div(c, n_half), 0, part] = out[:, :model_dim].astype(BF16)
        xds_ref[lax.div(c, n_half), 1, part] = out[:, model_dim:2 * model_dim].astype(BF16)
        sorted_gates[pl.ds(pl.multiple_of(c * CHUNK, CHUNK), CHUNK)] = out[:, 2 * model_dim:]

    order_rows(rank_ref[...], table, store)
    split = sorted_gates[...].T
    gate = split[:n_exp] + split[n_exp:2 * n_exp] + split[2 * n_exp:3 * n_exp]
    for i in range(n_exp):
        gate_ref[i] = gate[i:i + 1]

    lane = iota((n_exp, LANES), 1)
    hit = jnp.zeros((n_exp, LANES), F32)
    for t in range(n_tile):
        active = ones_where(jnp.max(gate[:, t * TILE:(t + 1) * TILE], axis=1, keepdims=True) > 0.0)
        hit = hit + jnp.where(lane == t, jnp.broadcast_to(active, (n_exp, LANES)), 0.0)
    row_a, row_b = iota((n_exp, n_exp), 0), iota((n_exp, n_exp), 1)
    row = iota((n_exp, LANES), 0)

    order, total = item_lists(hit, n_tile, jnp.ones((n_exp, n_exp), F32), row.astype(F32))
    near = jnp.sum(jnp.sum(jnp.where(row < n_exp - n_local, hit, 0.0), axis=1, keepdims=True), axis=0, keepdims=True)
    meta_ref[0:1] = order[0:1].astype(I32)
    meta_ref[1:2] = total[0:1].astype(I32)
    own = jnp.sum(jnp.sum(jnp.where(row < n_local, hit, 0.0), axis=1, keepdims=True), axis=0, keepdims=True)
    own = jnp.minimum(own, OWN_BLOCKS)
    meta_ref[2:3] = jnp.broadcast_to(own, (1, LANES)).astype(I32)
    meta_ref[3:4] = jnp.broadcast_to(jnp.minimum(near, own + HEAD_BLOCKS), (1, LANES)).astype(I32)
    order, total = item_lists(hit, n_tile, ones_where(row_a // n_local == row_b // n_local), lax.rem(row, n_local).astype(F32))
    pay_ref[...] = jnp.zeros_like(pay_ref)
    for s in range(n_exp // n_local):
        pay_ref[s, :n_local] = gate[s * n_local:(s + 1) * n_local]
        pay_ref[s, n_local:n_local + 1, :LANES] = order[s * n_local:s * n_local + 1]
        pay_ref[s, n_local + 1:n_local + 2, :LANES] = total[s * n_local:s * n_local + 1]


def local_kernel(n_parts, phase, *refs):
    last = phase == 2
    it = iter(refs)
    meta_ref, xf_ref, xd_ref, gate_ref = (next(it) for _ in range(4))
    parts = [next(it) for _ in range(n_parts)]
    if phase:
        y_in, dx_in = next(it), next(it)
    rank_ref = next(it) if last else None
    next(it)
    y_ref, dx_ref, token_ref = next(it), next(it), next(it)
    token_ref[...] = jnp.zeros_like(token_ref)
    w, sems = next(it), next(it)
    if last:
        y_acc, dx_acc, rank_col, table = (next(it) for _ in range(4))
    else:
        y_acc, dx_acc = y_ref, dx_ref
    n_tok, model_dim = xf_ref.shape

    copies = []
    at = 0
    for part in parts:
        n = part.shape[0]
        copies.append(pltpu.make_async_copy(part, w.at[pl.ds(at, n)], sems.at[len(copies)]))
        at += n
    for c in copies:
        c.start()
    if phase:
        y_acc[...] = y_in[...]
        dx_acc[...] = dx_in[...]
    else:
        y_acc[...] = jnp.zeros_like(y_acc)
        dx_acc[...] = jnp.zeros_like(dx_acc)
    for c in copies:
        c.wait()

    n_half = n_tok // 2 // TILE

    bounds = 0, meta_ref[2, 0], meta_ref[3, 0], meta_ref[1, 0]
    begin, end = bounds[phase], bounds[phase + 1]

    def chain(k):
        m = meta_ref[0, jnp.minimum(k, end - 1)]
        e, r = lax.div(m, n_tok // TILE), lax.rem(m, n_tok // TILE)
        rows = pl.ds(pl.multiple_of(r * TILE, TILE), TILE)
        part = pl.ds(pl.multiple_of(lax.rem(r, n_half) * TILE, TILE), TILE)
        half = lax.div(r, n_half)
        x_f, x_b, dy = xf_ref[rows], xd_ref[half, 0, part], xd_ref[half, 1, part]
        w1, w3, w2t = w[e, 0], w[e, 1], w[e, 2]
        gate_row = gate_ref[e, :, rows] * (k < end).astype(F32)
        gate = jnp.broadcast_to(gate_row, (model_dim, TILE)).T
        a1, a3 = dot(x_f, w1), dot(x_f, w3)
        h = (a1 * sigmoid(a1) * a3).astype(BF16)
        y = gate * dot_nt(h, w2t).astype(BF16).astype(F32)
        d = (gate * dy.astype(F32)).astype(BF16)
        b1, b3 = dot(x_b, w1), dot(x_b, w3)
        dh = dot(d, w2t).astype(BF16).astype(F32)
        sg = sigmoid(b1)
        act = b1 * sg
        d3 = (dh * act).astype(BF16)
        d1 = (dh * b3 * (sg + act * (1.0 - sg))).astype(BF16)
        dx = (dot_nt(d1, w1) + dot_nt(d3, w3)).astype(BF16).astype(F32)
        return rows, y, dx

    def blocks(p, _):
        for rows, y, dx in [chain(begin + LOCAL_BLOCKS * p + k) for k in range(LOCAL_BLOCKS)]:
            y_acc[rows] += y
            dx_acc[rows] += dx
        return 0

    lax.fori_loop(0, lax.div(end - begin + LOCAL_BLOCKS - 1, LOCAL_BLOCKS), blocks, 0)

    if last:
        rank_col[...] = jnp.broadcast_to(rank_ref[...], (LANES, n_tok)).T
        table[:, :model_dim] = y_acc[...].astype(BF16)
        table[:, model_dim:] = dx_acc[...].astype(BF16)

        def restore(c, _):
            rows = pl.ds(pl.multiple_of(c * CHUNK, CHUNK), CHUNK)
            col = rank_col[rows, :]
            pick = jnp.concatenate([ones_where(col == iota((CHUNK, LANES), 1) + j * LANES).astype(BF16) for j in range(n_tok // LANES)], axis=1)
            out = dot(pick, table[...])
            y_ref[rows] = out[:, :model_dim].astype(BF16)
            dx_ref[rows] = out[:, model_dim:].astype(BF16)
            return 0

        lax.fori_loop(0, n_tok // CHUNK, restore, 0)


def owner_kernel(n_src, n_cut, first, last, *refs):
    it = iter(refs)
    meta_ref = next(it)
    sources = [[[next(it) for _ in range(n_cut)], next(it)] for _ in range(n_src)]
    w_ref = next(it)
    acc_in = None if first else [next(it) for _ in range(3)]
    next(it)
    outs = [next(it) for _ in range(3)]
    token_ref = next(it)
    token_ref[...] = jnp.zeros_like(token_ref)
    accs = [next(it) for _ in range(3)] if last else outs
    xd, pay, sems = next(it), next(it), next(it)
    copies = []
    for s, (xd_refs, pay_ref) in enumerate(sources):
        n = 2 // n_cut
        for k, ref in enumerate(xd_refs):
            copies.append(pltpu.make_async_copy(ref, xd.at[s, pl.ds(k * n, n)], sems.at[len(copies)]))
        copies.append(pltpu.make_async_copy(pay_ref, pay.at[s], sems.at[len(copies)]))
    for c in copies:
        c.start()
    n_local = w_ref.shape[0]
    acc1, acc3, acc2 = accs
    n_part = xd.shape[3] // TILE
    n_tile = 2 * n_part

    for k, acc in enumerate(accs):
        acc[...] = jnp.zeros_like(acc) if first else acc_in[k][...]
    for c in copies:
        c.wait()

    def chain(s, k, count):
        m = meta_ref[2 * s, k]
        e, t = lax.div(m, n_tile), lax.rem(m, n_tile)
        rows = pl.ds(pl.multiple_of(t * TILE, TILE), TILE)
        part = pl.ds(pl.multiple_of(lax.rem(t, n_part) * TILE, TILE), TILE)
        half = lax.div(t, n_part)
        x_t = xd[s, half, 0, part].T
        gate_row = pay[s, pl.ds(e, 1), rows] * (k < count).astype(F32)
        d_t = (gate_row * xd[s, half, 1, part].astype(F32).T).astype(BF16)
        a1, a3 = dot(w_ref[e, 0], x_t), dot(w_ref[e, 1], x_t)
        dh = dot(w_ref[e, 2], d_t).astype(BF16).astype(F32)
        sg = sigmoid(a1)
        act = a1 * sg
        h = (act * a3).astype(BF16)
        d3 = (dh * act).astype(BF16)
        d1 = (dh * a3 * (sg + act * (1.0 - sg))).astype(BF16)
        return e, dot_nt(d1, x_t), dot_nt(d3, x_t), dot_nt(h, d_t)

    def source(s, _):
        count = meta_ref[2 * s + 1, 0]

        def blocks(p, _):
            for e, g1, g3, g2 in [chain(s, OWNER_BLOCKS * p + k, count) for k in range(OWNER_BLOCKS)]:
                acc1[e] += g1
                acc3[e] += g3
                acc2[e] += g2
            return 0

        lax.fori_loop(0, lax.div(count + OWNER_BLOCKS - 1, OWNER_BLOCKS), blocks, 0)
        return 0

    lax.fori_loop(0, n_src, source, 0)

    if last:
        for e in range(n_local):
            outs[0][e] = acc1[e].astype(BF16).T
            outs[1][e] = acc3[e].astype(BF16).T
            outs[2][e] = acc2[e].astype(BF16)


VMEM = pl.BlockSpec(memory_space=pltpu.VMEM)
SMEM = pl.BlockSpec(memory_space=pltpu.SMEM)
ANY = pl.BlockSpec(memory_space=pl.ANY)
TOKEN = jax.ShapeDtypeStruct((8, LANES), F32)


def params(flops, mib=24):
    return dict(cost_estimate=pl.CostEstimate(flops=flops, bytes_accessed=8 << 20, transcendentals=0), compiler_params=pltpu.CompilerParams(vmem_limit_bytes=mib << 20))


def rank_call(aux, me, n_local, n_tok):
    return pl.pallas_call(
        functools.partial(rank_kernel, n_local),
        in_specs=[SMEM, VMEM],
        out_specs=[VMEM] * 3,
        out_shape=[jax.ShapeDtypeStruct((n_tok, LANES), BF16), jax.ShapeDtypeStruct((1, n_tok), I32), TOKEN],
        scratch_shapes=[pltpu.VMEM((n_tok, LANES), I32)],
        name='rank_tokens',
        **params(1 << 30),
    )(me, aux)


def forward_call(x_f, rank, after):
    n_tok, model_dim = x_f.shape
    return pl.pallas_call(
        forward_kernel,
        in_specs=[VMEM, VMEM, ANY],
        out_specs=VMEM,
        out_shape=jax.ShapeDtypeStruct(x_f.shape, BF16),
        name='sort_forward',
        **params(2 * n_tok * n_tok * model_dim),
    )(x_f, rank, after)


def sort_call(x_b, dy, cols, rank, n_local):
    n_tok, model_dim = x_b.shape
    n_exp = N_DEV * n_local
    shapes = [jax.ShapeDtypeStruct((2, 2, n_tok // 2, model_dim), BF16), jax.ShapeDtypeStruct((n_exp, 1, n_tok), F32), jax.ShapeDtypeStruct((N_DEV, PAY_ROWS, n_tok), F32), jax.ShapeDtypeStruct((4, LANES), I32)]
    return pl.pallas_call(
        functools.partial(sort_kernel, n_local),
        in_specs=[VMEM] * 4,
        out_specs=[VMEM] * len(shapes),
        out_shape=shapes,
        scratch_shapes=[pltpu.VMEM((n_tok, 2 * model_dim + LANES), BF16), pltpu.VMEM((n_tok, LANES), F32)],
        name='sort_tokens',
        **params(6 * n_tok * n_tok * model_dim),
    )(x_b, dy, cols, rank)


def local_call(meta, rows, gates, parts, carry, rank, after):
    n_tok, model_dim = rows[0].shape
    ffn = parts[0].shape[3]
    n_held = sum(p.shape[0] for p in parts)
    last = rank is not None
    args = [meta, *rows, gates, *parts]
    specs = [SMEM] + [VMEM] * 3 + [ANY] * len(parts)
    if carry is not None:
        args += list(carry)
        specs += [VMEM] * 2
    if last:
        args += [rank]
        specs += [VMEM]
    scratch = [pltpu.VMEM((n_held, 3, model_dim, ffn), BF16), pltpu.SemaphoreType.DMA((len(parts),))]
    if last:
        scratch += [pltpu.VMEM((n_tok, model_dim), F32)] * 2 + [pltpu.VMEM((n_tok, LANES), I32), pltpu.VMEM((n_tok, 2 * model_dim), BF16)]
    return pl.pallas_call(
        functools.partial(local_kernel, len(parts), 2 if last else 0 if carry is None else 1),
        in_specs=specs + [ANY],
        out_specs=[VMEM] * 3,
        out_shape=[jax.ShapeDtypeStruct((n_tok, model_dim), BF16 if last else F32)] * 2 + [TOKEN],
        scratch_shapes=scratch,
        **params(8 * n_tok * n_held * model_dim * ffn),
    )(*args, after)


def owner_call(meta, sources, weights, carry, last, after):
    n_local, _, ffn, model_dim = weights.shape
    n_cut = len(sources[0][0])
    cut, pay = sources[0][0][0], sources[0][1]
    args = [meta] + [a for s in sources for a in (*s[0], s[1])] + [weights]
    specs = [SMEM] + [ANY] * (len(args) - 2) + [VMEM]
    held = [pltpu.VMEM((len(sources), 2, *cut.shape[1:]), BF16), pltpu.VMEM((len(sources), *pay.shape), F32), pltpu.SemaphoreType.DMA((len(args) - 2,))]
    if carry is not None:
        args += list(carry)
        specs += [VMEM] * 3
    total = (n_local, ffn, model_dim)
    w_in = jax.ShapeDtypeStruct((n_local, model_dim, ffn), BF16)
    shapes = [w_in, w_in, jax.ShapeDtypeStruct(total, BF16)] if last else [jax.ShapeDtypeStruct(total, F32)] * 3
    return pl.pallas_call(
        functools.partial(owner_kernel, len(sources), n_cut, carry is None, last),
        in_specs=specs + [ANY],
        out_specs=[VMEM] * 4,
        out_shape=shapes + [TOKEN],
        scratch_shapes=([pltpu.VMEM(total, F32)] * 3 if last else []) + held,
        **params(6 * len(sources) * sources[0][1].shape[1] * n_local * model_dim * ffn),
    )(*args, after)


def pack_kernel(w1_ref, w3_ref, w2_ref, packed_ref, turned_ref, token_ref, packed, turned, sems):
    ins = [
        pltpu.make_async_copy(w2_ref, turned.at[:, 2], sems.at[0]),
        pltpu.make_async_copy(w1_ref, packed.at[:, 0], sems.at[1]),
        pltpu.make_async_copy(w3_ref, packed.at[:, 1], sems.at[2]),
    ]
    outs = [pltpu.make_async_copy(packed, packed_ref, sems.at[3]), pltpu.make_async_copy(turned, turned_ref, sems.at[4])]
    for c in ins:
        c.start()
    token_ref[...] = jnp.zeros_like(token_ref)
    ins[0].wait()
    for e in range(packed.shape[0]):
        packed[e, 2] = turned[e, 2].T
    ins[1].wait()
    ins[2].wait()
    outs[0].start()
    for e in range(packed.shape[0]):
        turned[e, 0] = packed[e, 0].T
        turned[e, 1] = packed[e, 1].T
    outs[1].start()
    for c in outs:
        c.wait()


def pack_call(w1, w3, w2):
    n, model_dim, ffn = w1.shape
    shapes = (n, 3, model_dim, ffn), (n, 3, ffn, model_dim)
    return pl.pallas_call(
        pack_kernel,
        in_specs=[ANY] * 3,
        out_specs=[ANY] * 2 + [VMEM],
        out_shape=[jax.ShapeDtypeStruct(shape, BF16) for shape in shapes] + [TOKEN],
        scratch_shapes=[pltpu.VMEM(shape, BF16) for shape in shapes] + [pltpu.SemaphoreType.DMA((5,))],
        name='pack_weights',
        **params(1 << 20, 62),
    )(w1, w3, w2)


def halves_kernel(left_ref, right_ref, after_ref, head_ref, tail_ref, token_ref):
    head_ref[...] = left_ref[...]
    tail_ref[...] = right_ref[...]
    token_ref[...] = jnp.zeros_like(token_ref)


def halves_call(left, right, after):
    shape = (left.shape[0] // 2, *left.shape[1:])
    rest = (0,) * (left.ndim - 1)
    first, second = pl.BlockSpec(shape, lambda i: (0, *rest)), pl.BlockSpec(shape, lambda i: (1, *rest))
    return pl.pallas_call(
        halves_kernel,
        grid=(1,),
        in_specs=[first, second, ANY],
        out_specs=[first, first, VMEM],
        out_shape=[jax.ShapeDtypeStruct(shape, left.dtype)] * 2 + [TOKEN],
        name='halves',
        **params(1 << 20),
    )(left, right, after)


def solution(mesh):
    n_stage = mesh.shape['stage']
    n_dev = mesh.shape['expert']
    assert n_dev == N_DEV
    to_next = [(i, (i + 1) % n_stage) for i in range(n_stage)]
    to_prev = [((i + 1) % n_stage, i) for i in range(n_stage)]
    tok_spec = P('stage', 'expert', None)
    w_spec = P('stage', 'expert', None, None)

    def from_ring(a, ahead):
        return lax.ppermute(a, 'expert', [((i + ahead) % n_dev, i) for i in range(n_dev)])

    def from_sides(a):
        return from_ring(a, n_dev - 1), from_ring(a, 1)

    def from_far(sides, after):
        head, tail, token = halves_call(*sides, after)
        return (from_ring(head, n_dev - 1), from_ring(tail, 1)), token

    def moe_layer(x_act, route_idx, route_wts, w_one, w_three, w_two, dy_act):
        x_src, dy = x_act[0], dy_act[0]
        n_local = w_one.shape[1]
        me = lax.axis_index('expert').astype(I32).reshape(1)

        aux = jnp.concatenate([route_idx[0].T.astype(F32), route_wts[0].T], axis=0)
        aux, w1 = lax.optimization_barrier((aux, w_one[0]))
        packed, turned, pack_token = pack_call(w1, w_three[0], w_two[0])
        aux = lax.ppermute(aux, 'stage', to_next)
        x_b = lax.ppermute(x_src, 'stage', to_next)
        x_again, aux, pack_token = lax.optimization_barrier((x_src, aux, pack_token))
        x_f = lax.ppermute(x_again, 'stage', to_next)
        sides = from_sides(packed)
        cols, rank, rank_token = rank_call(aux, me, n_local, x_src.shape[0])
        xd, gates, pay, meta = sort_call(x_b, dy, cols, rank, n_local)
        pay_side = from_ring(pay[2], n_dev - 1), from_ring(pay[1], 1)
        pay_far = from_ring(pay[3], 2)
        xd_side = from_sides(xd)

        def lists(after, *pays):
            return jnp.concatenate([p[n_local:n_local + 2, :LANES] + after[:2] for p in pays], axis=0).astype(I32)

        *sums, token = owner_call(lists(rank_token, pay[0]), [((xd,), pay[0])], turned, None, False, rank_token)
        rows = (forward_call(x_f, rank, token), xd)
        *totals, token = local_call(meta, rows, gates, [packed], None, None, token)
        far, token = from_far(sides, token)
        *totals, token = local_call(meta, rows, gates, [packed, *sides], totals, None, token)
        xd_far, token = from_far(xd_side, token)
        *sums, token = owner_call(lists(token, *pay_side), [((xd_side[k],), pay_side[k]) for k in range(2)], turned, sums, False, token)
        y, dx, token = local_call(meta, rows, gates, [packed, *sides, *far], totals, rank, token)
        dx_src = lax.ppermute(dx, 'stage', to_prev)
        g_one, g_three, g_two, token = owner_call(lists(token, pay_far), [(xd_far, pay_far)], turned, sums, True, token)
        return y[None], dx_src[None], g_one[None], g_three[None], g_two[None]

    return jax.shard_map(moe_layer, mesh=mesh, in_specs=(tok_spec, tok_spec, tok_spec, w_spec, w_spec, w_spec, tok_spec), out_specs=(tok_spec, tok_spec, w_spec, w_spec, w_spec), check_vma=False)
```
